768 devices in a mesh: dp: 32 (over z_hi, x, core), tensor: 24 (over z_lo, y).
Axes of the slice: x: 4, y: 8, z: 12 (z_hi: 4, z_lo: 3; z = z_hi * 3 + z_lo), core: 2. Of those that a mesh axis runs over, the one named last changes fastest.
Arguments:
- saved_input: bfloat16 [8192, 6144], P('dp', 'tensor'), may hold values from -6 to 6
- queries: bfloat16 [8192, 6144], P('dp', 'tensor'), may hold values from -8 to 8
- keys: bfloat16 [8192, 6144], P('dp', 'tensor'), may hold values from -8 to 8
- value_weight: bfloat16 [6144, 6144], P(None, 'tensor'), may hold values from -0.125 to 0.125
- grad_attended: bfloat16 [8192, 6144], P('dp', 'tensor'), may hold values from -6 to 6
Outputs:
- grad_input: bfloat16 [8192, 6144], P('dp', 'tensor')
- grad_value_weight: float32 [6144, 6144], P('dp', 'tensor')
- grad_queries: bfloat16 [8192, 6144], P('dp', 'tensor')
- grad_keys: bfloat16 [8192, 6144], P('dp', 'tensor')
The draws below stay inside these ranges and needn't reach their ends.
All inputs are finite; a program needn't handle non-finite values.
Results may differ from the reference program's by a relative error of at most 0.02.
Values may be sent and summed in bfloat16 or wider, within the bound.
A program may use at most 64 MiB of HBM per device.

```python
import jax
import jax.numpy as jnp
from jax import lax

D = 6144
HD = 128
HEADS_DEV = 2
SEQ = 256
HEADS = 48
GROUPS = 32
TOKENS = 8192


def paired_fields(key):
    query_seed, key_seed = jax.random.split(jax.random.fold_in(key, 7919))
    field_shape = (TOKENS, HEADS, HD)
    query_field = jax.random.truncated_normal(query_seed, -5.0, 5.0, field_shape, jnp.float32)
    key_field = jax.random.truncated_normal(key_seed, -5.0, 5.0, field_shape, jnp.float32)
    total_width = HEADS * HD
    return (query_field.reshape(TOKENS, total_width).astype(jnp.bfloat16), key_field.reshape(TOKENS, total_width).astype(jnp.bfloat16))


def draw_queries(key, part):
    return paired_fields(key)[0]


def draw_keys(key, part):
    return paired_fields(key)[1]


def strengthened(drawn, rng, source, target, parts, factor):
    owner, partner = [(jnp.arange(drawn.shape[dim]) // (drawn.shape[dim] // parts)).reshape([-1 if axis == dim else 1 for axis in range(drawn.ndim)]) for dim in (source, target)]
    chosen = jax.random.permutation(rng, parts)[partner]
    strong = (owner == chosen) | (owner == (partner + parts // 2) % parts)
    return jnp.where(strong, factor * drawn, drawn)


def block_levels(key, dims, cuts, low, largest):
    factor_of, own = 1.0, jax.random.fold_in(key, 6)
    for axis_at, blocks in cuts:
        steps = jnp.exp(jax.random.uniform(jax.random.fold_in(own, axis_at), (blocks,), jnp.float32, low / len(cuts), largest / len(cuts)))
        factor_of = factor_of * jnp.repeat(steps, dims[axis_at] // blocks).reshape([-1 if axis == axis_at else 1 for axis in range(len(dims))])
    return factor_of


def bell_draw(key, shape, width, reach, shards=(), kind=jnp.bfloat16):
    loudness = block_levels(key, shape, shards, -0.22, 0.18) if shards else 1.0
    values = jax.random.normal(key, shape, jnp.float32) * width * loudness
    return jnp.minimum(jnp.maximum(values, -reach), reach).astype(kind)


def bell_draw_with(rng, extent, width, most, shards, heavy, kind=jnp.bfloat16):
    entries = width * jax.random.normal(rng, extent, jnp.float32)
    if shards:
        entries = entries * block_levels(rng, extent, shards, -0.22, 0.18)
    return jnp.clip(strengthened(entries, jax.random.fold_in(rng, 3), *heavy), -most, most).astype(kind)


def setup_inputs(seed: int = 0) -> dict:
    key_list = jax.random.split(jax.random.key(seed), 6)
    saved_input = bell_draw_with(key_list[0], (TOKENS, D), 1.0, 6.0, ((0, 32), (1, 24)), (0, 1, 32, 2.75))
    queries = draw_queries(jax.random.fold_in(key_list[5], 71), 0)
    keys = draw_keys(jax.random.fold_in(key_list[5], 71), 0)
    value_weight = bell_draw_with(key_list[3], (D, HEADS * HD), D ** -0.5, 0.125, ((1, 24),), (1, 0, 24, 2.25))
    grad_attended = bell_draw(key_list[4], (TOKENS, HEADS * HD), 1.0, 6.0, ((0, 32), (1, 24)))
    return dict(saved_input=saved_input, queries=queries, keys=keys, value_weight=value_weight, grad_attended=grad_attended)


def attention_backward(group_query, group_key, group_values, group_grad, causal):
    score_scale = 1.0 / jnp.sqrt(jnp.float32(HD))
    query_heads = group_query.astype(jnp.float32).reshape(SEQ, HEADS, HD)
    key_heads = group_key.astype(jnp.float32).reshape(SEQ, HEADS, HD)
    value_heads = group_values.astype(jnp.float32).reshape(SEQ, HEADS, HD)
    grad_heads = group_grad.astype(jnp.float32).reshape(SEQ, HEADS, HD)
    scores = jnp.einsum('qhd,khd->hqk', query_heads, key_heads) * score_scale
    scores = jnp.where(causal[None], scores, -jnp.inf)
    row_max = lax.optimization_barrier(jnp.max(scores, axis=-1, keepdims=True))
    weights_exp = jnp.exp(scores - row_max)
    attention = weights_exp / lax.optimization_barrier(jnp.sum(weights_exp, axis=-1, keepdims=True))
    probs_half = attention.astype(jnp.bfloat16).astype(jnp.float32)
    grad_values = jnp.einsum('hqk,qhd->khd', probs_half, grad_heads).astype(jnp.bfloat16)
    grad_probs = jnp.einsum('qhd,khd->hqk', grad_heads, value_heads)
    row_dot = lax.optimization_barrier(jnp.sum(attention * grad_probs, axis=-1, keepdims=True))
    grad_scores = (attention * (grad_probs - row_dot) * score_scale).astype(jnp.bfloat16).astype(jnp.float32)
    grad_queries = jnp.einsum('hqk,khd->qhd', grad_scores, key_heads).astype(jnp.bfloat16)
    grad_keys = jnp.einsum('hqk,qhd->khd', grad_scores, query_heads).astype(jnp.bfloat16)
    total_width = HEADS * HD
    return (grad_values.reshape(SEQ, total_width), grad_queries.reshape(SEQ, total_width), grad_keys.reshape(SEQ, total_width))

def reference(saved_input, queries, keys, value_weight, grad_attended):
    total_width = HEADS * HD
    block_width = HEADS_DEV * HD
    block_count = total_width // block_width
    weight_blocks = value_weight.astype(jnp.float32).reshape(D, block_count, block_width)
    positions = jnp.arange(SEQ)
    causal = positions[:, None] >= positions[None, :]

    def one_group(total, inputs):
        group_input, group_query, group_key, group_grad = inputs
        values = jnp.dot(group_input, value_weight, preferred_element_type=jnp.float32).astype(jnp.bfloat16)
        grad_values, grad_queries, grad_keys = attention_backward(group_query, group_key, values, group_grad, causal)
        value_blocks = grad_values.astype(jnp.float32).reshape(SEQ, block_count, block_width)
        partial_value = jnp.einsum('tnc,dnc->ntd', value_blocks, weight_blocks)
        partial_value = lax.optimization_barrier(partial_value.astype(jnp.bfloat16)).astype(jnp.float32)
        grad_input = lax.optimization_barrier(jnp.sum(partial_value, axis=0)).astype(jnp.bfloat16)
        weight_term = jnp.dot(group_input.T, grad_values, preferred_element_type=jnp.float32)
        weight_term = lax.optimization_barrier(weight_term.astype(jnp.bfloat16)).astype(jnp.float32)
        return (total + weight_term, (grad_input, grad_queries, grad_keys))
    stacked = (saved_input.reshape(GROUPS, SEQ, D), queries.reshape(GROUPS, SEQ, total_width), keys.reshape(GROUPS, SEQ, total_width), grad_attended.reshape(GROUPS, SEQ, total_width))
    total, results = lax.scan(one_group, jnp.zeros((D, total_width), jnp.float32), stacked)
    grad_input, grad_queries, grad_keys = results
    grad_value_weight = total / jnp.float32(GROUPS)
    return (grad_input.reshape(TOKENS, D), grad_value_weight, grad_queries.reshape(TOKENS, total_width), grad_keys.reshape(TOKENS, total_width))
```

```python
import math

import jax
import jax.numpy as jnp
from jax import lax
from jax.experimental import pallas as pl
from jax.experimental.pallas import tpu as pltpu
from jax.sharding import Mesh
from jax.sharding import PartitionSpec as P

HD = 128
HEADS = 2
ZH, X, C, ZL, Y = 4, 4, 2, 3, 8
AXES = ("zh", "x", "c", "zl", "y")
T = ZL * Y
B = 256
H = B // 2
MESH = pl.DeviceIdType.MESH
F32 = jnp.float32
BF16 = jnp.bfloat16
SCALE = 1.0 / math.sqrt(HD)


def dot(a, b, ca, cb):
    return lax.dot_general(a, b, (((ca,), (cb,)), ((), ())), preferred_element_type=F32)


def kernel(
    x_hbm, q_hbm, k_hbm, w_hbm, ga_hbm,
    gi_ref, gw_ref, gq_ref, gk_ref,
    xall, w, q, k, ga, gv, att, vals, acc0, acc1,
    wt, crecv, abuf, xr1, xr2, bbuf, zr1, zr2,
    s4_out, s4_in, rs_out, rs_in, tz_out, tz_in,
    in_sem, agz_s, agz_r, ag_s, ag_r, rs_s, rs_r, tz_s, tz_r,
    c_s, c_r, x1_s, x1_r, x2_s, x2_r, z1_s, z1_r, z2_s, z2_r,
):
    zh, xx, c, zl, y = (lax.axis_index(a) for a in AXES)
    me = zl * Y + y
    acc = (acc0, acc1)

    def up(value, step, size):
        return lax.rem(value + (step + size), size)

    ahead = ({"y": up(y, 1, Y)}, {"y": up(y, -1, Y)})
    x_side = ({"x": up(xx, 1, X)}, {"x": up(xx, -1, X)})
    z_side = ({"zh": up(zh, 1, ZH)}, {"zh": up(zh, -1, ZH)})
    plane = ({"zl": up(zl, 1, ZL)}, {"zl": up(zl, 2, ZL)})
    partner = {"c": 1 - c}

    def remote(src, dst, send, recv, where):
        return pltpu.make_async_remote_copy(
            src_ref=src, dst_ref=dst, send_sem=send, recv_sem=recv,
            device_id=where, device_id_type=MESH,
        )

    loads = [
        pltpu.make_async_copy(x_hbm, xall.at[me], in_sem.at[0]),
        pltpu.make_async_copy(q_hbm, q, in_sem.at[1]),
        pltpu.make_async_copy(k_hbm, k, in_sem.at[2]),
        pltpu.make_async_copy(ga_hbm, ga, in_sem.at[3]),
        pltpu.make_async_copy(w_hbm, w, in_sem.at[4]),
    ]
    for load in loads:
        load.start()

    barrier = pltpu.get_barrier_semaphore()
    friends = (*ahead, *x_side, *z_side, *plane, partner)
    for friend in friends:
        pl.semaphore_signal(barrier, inc=1, device_id=friend, device_id_type=MESH)
    pl.semaphore_wait(barrier, len(friends))

    def near(kk):
        return up(zl, -kk, ZL)

    def ag_full(d, s, kk, t):
        return remote(xall.at[t], xall.at[t], ag_s.at[d, s, kk], ag_r.at[d, s, kk], ahead[d])

    def ag_half(d, kk, t):
        part = pl.ds(d * H, H)
        return remote(
            xall.at[t, part], xall.at[t, part], ag_s.at[d, 3, kk], ag_r.at[d, 3, kk], ahead[d]
        )

    def ag_z(j, t):
        return remote(xall.at[t], xall.at[t], agz_s.at[j], agz_r.at[j], plane[j])

    loads[0].wait()
    for j in range(2):
        ag_z(j, me).start()
    for d in range(2):
        ag_full(d, 0, 0, me).start()

    row = lax.broadcasted_iota(jnp.int32, (B, B), 0)
    col = lax.broadcasted_iota(jnp.int32, (B, B), 1)
    for load in loads[1:4]:
        load.wait()

    def probs(h):
        cols = slice(h * HD, (h + 1) * HD)
        scores = dot(q[:, cols], k[:, cols], 1, 1) * SCALE
        scores = jnp.where(row >= col, scores, -jnp.inf)
        e = jnp.exp(scores - jnp.max(scores, axis=-1, keepdims=True))
        a = e / jnp.sum(e, axis=-1, keepdims=True)
        att[h] = a
        gv[:, cols] = dot(a.astype(BF16), ga[:, cols], 0, 0).astype(BF16)

    probs(0)
    for j in range(2):
        t = near(j + 1) * Y + y
        ag_z(j, t).wait_recv()
        for d in range(2):
            ag_full(d, 0, j + 1, t).start()
    probs(1)
    vals[...] = jnp.zeros_like(vals)
    loads[4].wait()

    def consume(t):
        rows = pl.ds(pl.multiple_of(t * B, B), B)
        vals[...] += dot(xall[t], w[rows], 1, 0)
        term = dot(xall[t], gv[...], 0, 0).astype(BF16)
        wt[pl.ds(t * 4, 4)] = term.reshape(4, 64, B)

    def own_chunks(kk, carry):
        consume(near(kk) * Y + y)
        return carry

    lax.fori_loop(0, ZL, own_chunks, 0)

    def ring(i, carry):
        s = i // ZL
        kk = lax.rem(i, ZL)
        ts = (near(kk) * Y + up(y, -(s + 1), Y), near(kk) * Y + up(y, s + 1, Y))
        for d in range(2):
            ag_full(d, s, kk, ts[d]).wait_recv()

            @pl.when(s < 2)
            def _():
                ag_full(d, s + 1, kk, ts[d]).start()

            @pl.when(s == 2)
            def _():
                ag_half(d, kk, ts[d]).start()

        for d in range(2):
            consume(ts[d])
        return carry

    lax.fori_loop(0, 3 * ZL, ring, 0)

    def far(kk):
        return up(zl, kk + 1, ZL)

    def share(t):
        rows = pl.ds(pl.multiple_of(t * B, B), B)
        return dot(gv[...], w[rows], 1, 1)

    def rs_half(d, kk):
        return remote(
            s4_out.at[d, kk], s4_in.at[d, kk], rs_s.at[d, 0, kk], rs_r.at[d, 0, kk], ahead[d]
        )

    def rs_full(d, n, kk):
        return remote(
            rs_out.at[d, n, kk], rs_in.at[d, n, kk],
            rs_s.at[d, n + 1, kk], rs_r.at[d, n + 1, kk], ahead[d],
        )

    def rs_z(j):
        return remote(tz_out.at[j], tz_in.at[j], tz_s.at[j], tz_r.at[j], plane[j])

    def rs_first(kk, carry):
        p = share(far(kk) * Y + up(y, 4, Y)).astype(BF16)
        for d in range(2):
            s4_out[d, kk] = p[d * H : (d + 1) * H]
            rs_half(d, kk).start()
        return carry

    lax.fori_loop(0, ZL, rs_first, 0)

    def last_chunks(kk, carry):
        t = near(kk) * Y + up(y, 4, Y)
        for d in range(2):
            ag_half(d, kk, t).wait_recv()
        consume(t)
        return carry

    lax.fori_loop(0, ZL, last_chunks, 0)

    def c_send(i):
        other = (2 * i + 1 - c) * 3
        return remote(wt.at[pl.ds(other, 3)], crecv.at[i], c_s.at[i], c_r.at[i], partner)

    def x_first(d):
        return remote(
            abuf.at[pl.ds(2 * d, 2), up(xx, 2, X)], xr1.at[d], x1_s.at[d], x1_r.at[d], x_side[d]
        )

    def x_second(d):
        return remote(
            abuf.at[:, x_side[d]["x"]], xr2.at[d], x2_s.at[d], x2_r.at[d], x_side[d]
        )

    def z_first(d):
        return remote(
            bbuf.at[up(zh, 2, ZH), :, pl.ds(32 * d, 32)], zr1.at[d],
            z1_s.at[d], z1_r.at[d], z_side[d],
        )

    def z_second(d):
        return remote(
            bbuf.at[z_side[d]["zh"]], zr2.at[d], z2_s.at[d], z2_r.at[d], z_side[d]
        )

    def cores(i, carry):
        c_send(i).start()
        return carry

    lax.fori_loop(0, ZH * X, cores, 0)

    def pair_sum(j, carry):
        to = up(xx, 2 + j // ZH, X)
        i = lax.rem(j, ZH) * X + to
        c_send(i).wait_recv()
        mine = wt[pl.ds((2 * i + c) * 3, 3)].astype(F32)
        abuf[lax.rem(j, ZH), to] = (mine + crecv[i].astype(F32)).astype(BF16)
        return carry

    lax.fori_loop(0, ZH, pair_sum, 0)
    for d in range(2):
        x_first(d).start()
    lax.fori_loop(ZH, ZH * X, pair_sum, 0)

    def rs_block(n):
        step = 3 - n

        def body(kk, carry):
            for d in range(2):
                acc[d][...] = share(far(kk) * Y + up(y, step if d == 0 else -step, Y))
            for d in range(2):
                if n == 0:
                    rs_half(d, kk).wait_recv()
                    part = slice(d * H, (d + 1) * H)
                    acc[d][part] += s4_in[d, kk].astype(F32)
                    rs_out[d, n, kk] = acc[d][...].astype(BF16)
                else:
                    rs_full(d, n - 1, kk).wait_recv()
                    rs_out[d, n, kk] = (acc[d][...] + rs_in[d, n - 1, kk].astype(F32)).astype(BF16)
                rs_full(d, n, kk).start()
            return carry

        lax.fori_loop(0, ZL, body, 0)

    rs_block(0)

    def grads(h):
        cols = slice(h * HD, (h + 1) * HD)
        a = att[h]
        gp = dot(ga[:, cols], vals[:, cols].astype(BF16), 1, 1)
        rd = jnp.sum(a * gp, axis=-1, keepdims=True)
        gs = (a * (gp - rd) * SCALE).astype(BF16)
        gq_ref[:, cols] = dot(gs, k[:, cols], 1, 0).astype(BF16)
        gk_ref[:, cols] = dot(gs, q[:, cols], 0, 0).astype(BF16)

    for d in range(2):
        x_first(d).wait_recv()
        to = x_side[d]["x"]
        for half in range(2):
            m = 2 * d + half
            abuf[m, to] = (abuf[m, to].astype(F32) + xr1[d, half].astype(F32)).astype(BF16)
        x_second(d).start()

    rs_block(1)
    for d in range(2):
        x_second(d).wait_recv()

    def x_sum(m, carry):
        total = abuf[m, xx].astype(F32) + xr2[0, m].astype(F32) + xr2[1, m].astype(F32)
        bbuf[m] = total.astype(BF16)
        return carry

    lax.fori_loop(0, ZH, x_sum, 0)
    for d in range(2):
        z_first(d).start()
    grads(0)
    rs_block(2)
    for d in range(2):
        z_first(d).wait_recv()
        to = z_side[d]["zh"]
        part = slice(32 * d, 32 * (d + 1))
        bbuf[to, :, part] = (bbuf[to, :, part].astype(F32) + zr1[d].astype(F32)).astype(BF16)
        z_second(d).start()

    for kk in range(ZL):
        acc0[...] = share(far(kk) * Y + y)
        for d in range(2):
            rs_full(d, 2, kk).wait_recv()
        total = acc0[...] + rs_in[0, 2, kk].astype(F32) + rs_in[1, 2, kk].astype(F32)
        if kk < 2:
            tz_out[kk] = total.astype(BF16)
            rs_z(kk).start()
        else:
            acc0[...] = total
    grads(1)
    for j in range(2):
        rs_z(j).wait_recv()
    gi_ref[...] = (acc0[...] + tz_in[0].astype(F32) + tz_in[1].astype(F32)).astype(BF16)
    for d in range(2):
        z_second(d).wait_recv()
    total = bbuf[zh].astype(F32) + zr2[0].astype(F32) + zr2[1].astype(F32)
    gw_ref[...] = (total * F32(1.0 / (ZH * X * C))).reshape(192, B)

    for j in range(2):
        ag_z(j, me).wait_send()
        rs_z(j).wait_send()
    for d in range(2):
        x_first(d).wait_send()
        x_second(d).wait_send()
        z_first(d).wait_send()
        z_second(d).wait_send()

    def sent(kk, carry):
        for d in range(2):
            for s in range(3):
                ag_full(d, s, kk, me).wait_send()
                rs_full(d, s, kk).wait_send()
            ag_half(d, kk, me).wait_send()
            rs_half(d, kk).wait_send()
        return carry

    lax.fori_loop(0, ZL, sent, 0)

    def pair_sent(i, carry):
        c_send(i).wait_send()
        return carry

    lax.fori_loop(0, ZH * X, pair_sent, 0)


def on_device(saved_input, queries, keys, value_weight, grad_attended):
    hbm = pl.BlockSpec(memory_space=pltpu.HBM)
    vmem = pl.BlockSpec(memory_space=pltpu.VMEM)
    dma = pltpu.SemaphoreType.DMA
    outs = pl.pallas_call(
        kernel,
        out_shape=(
            jax.ShapeDtypeStruct((B, B), BF16),
            jax.ShapeDtypeStruct((192, B), F32),
            jax.ShapeDtypeStruct((B, B), BF16),
            jax.ShapeDtypeStruct((B, B), BF16),
        ),
        in_specs=[hbm] * 5,
        out_specs=(vmem,) * 4,
        scratch_shapes=[
            pltpu.VMEM((T, B, B), BF16),
            pltpu.VMEM((T * B, B), BF16),
            pltpu.VMEM((B, B), BF16),
            pltpu.VMEM((B, B), BF16),
            pltpu.VMEM((B, B), BF16),
            pltpu.VMEM((B, B), BF16),
            pltpu.VMEM((HEADS, B, B), F32),
            pltpu.VMEM((B, B), F32),
            pltpu.VMEM((B, B), F32),
            pltpu.VMEM((B, B), F32),
            pltpu.VMEM((T * 4, 64, B), BF16),
            pltpu.VMEM((ZH * X, 3, 64, B), BF16),
            pltpu.VMEM((ZH, X, 3, 64, B), BF16),
            pltpu.VMEM((2, 2, 3, 64, B), BF16),
            pltpu.VMEM((2, ZH, 3, 64, B), BF16),
            pltpu.VMEM((ZH, 3, 64, B), BF16),
            pltpu.VMEM((2, 3, 32, B), BF16),
            pltpu.VMEM((2, 3, 64, B), BF16),
            pltpu.VMEM((2, ZL, H, B), BF16),
            pltpu.VMEM((2, ZL, H, B), BF16),
            pltpu.VMEM((2, 3, ZL, B, B), BF16),
            pltpu.VMEM((2, 3, ZL, B, B), BF16),
            pltpu.VMEM((2, B, B), BF16),
            pltpu.VMEM((2, B, B), BF16),
            dma((5,)),
            dma((2,)), dma((2,)),
            dma((2, 4, ZL)), dma((2, 4, ZL)),
            dma((2, 4, ZL)), dma((2, 4, ZL)),
            dma((2,)), dma((2,)),
            dma((ZH * X,)), dma((ZH * X,)),
            dma((2,)), dma((2,)), dma((2,)), dma((2,)),
            dma((2,)), dma((2,)), dma((2,)), dma((2,)),
        ],
        compiler_params=pltpu.CompilerParams(
            collective_id=0, has_side_effects=True, vmem_limit_bytes=48 * 1024 * 1024
        ),
    )(saved_input, queries, keys, value_weight, grad_attended)
    return outs


def solution(mesh):
    torus = Mesh(mesh.devices.reshape(ZH, X, C, ZL, Y), AXES)
    rows, cols = ("zh", "x", "c"), ("zl", "y")
    placed = (P(rows, cols), P(rows, cols), P(rows, cols), P(None, cols), P(rows, cols))
    return jax.shard_map(
        on_device,
        mesh=torus,
        in_specs=placed,
        out_specs=(P(rows, cols),) * 4,
        check_vma=False,
    )
```

```python
import math

import jax
import jax.numpy as jnp
from jax import lax
from jax.experimental import pallas as pl
from jax.experimental.pallas import tpu as pltpu
from jax.sharding import Mesh
from jax.sharding import PartitionSpec as P

HD = 128
HEADS = 2
ZH, X, C, ZL, Y = 4, 4, 2, 3, 8
AXES = ("zh", "x", "c", "zl", "y")
T = ZL * Y
B = 256
H = B // 2
RA = 160
MESH = pl.DeviceIdType.MESH
F32 = jnp.float32
BF16 = jnp.bfloat16
SCALE = 1.0 / math.sqrt(HD)


def dot(a, b, ca, cb):
    return lax.dot_general(a, b, (((ca,), (cb,)), ((), ())), preferred_element_type=F32)


def kernel(
    x_hbm, q_hbm, k_hbm, w_hbm, ga_hbm,
    gi_ref, gw_ref, gq_ref, gk_ref,
    xall, w, q, k, ga, gv, att, vals, acc0, acc1,
    wt, crecv, abuf, xr1, xr2, bbuf, zr1, zr2,
    s4_out, s4_in, rs_out, rs_in, tz_out, tz_in,
    in_sem, agz_s, agz_r, agb_s, agb_r, ag_s, ag_r, rs_s, rs_r, tz_s, tz_r,
    c_s, c_r, x1_s, x1_r, x2_s, x2_r, z1_s, z1_r, z2_s, z2_r,
):
    zh, xx, c, zl, y = (lax.axis_index(a) for a in AXES)
    me = zl * Y + y
    acc = (acc0, acc1)

    def up(value, step, size):
        return lax.rem(value + (step + size), size)

    ahead = ({"y": up(y, 1, Y)}, {"y": up(y, -1, Y)})
    x_side = ({"x": up(xx, 1, X)}, {"x": up(xx, -1, X)})
    z_side = ({"zh": up(zh, 1, ZH)}, {"zh": up(zh, -1, ZH)})
    plane = ({"zl": up(zl, 1, ZL)}, {"zl": up(zl, 2, ZL)})
    partner = {"c": 1 - c}

    def remote(src, dst, send, recv, where):
        return pltpu.make_async_remote_copy(
            src_ref=src, dst_ref=dst, send_sem=send, recv_sem=recv,
            device_id=where, device_id_type=MESH,
        )

    loads = [
        pltpu.make_async_copy(x_hbm, xall.at[me], in_sem.at[0]),
        pltpu.make_async_copy(q_hbm, q, in_sem.at[1]),
        pltpu.make_async_copy(k_hbm, k, in_sem.at[2]),
        pltpu.make_async_copy(ga_hbm, ga, in_sem.at[3]),
        pltpu.make_async_copy(w_hbm, w, in_sem.at[4]),
    ]
    for load in loads:
        load.start()

    barrier = pltpu.get_barrier_semaphore()
    friends = (*ahead, *x_side, *z_side, *plane, partner)
    for friend in friends:
        pl.semaphore_signal(barrier, inc=1, device_id=friend, device_id_type=MESH)
    pl.semaphore_wait(barrier, len(friends))

    def near(kk):
        return up(zl, -kk, ZL)

    def ag_y(d, s, kk, t):
        n = B if kk == 0 else RA
        part = pl.ds(d * (n // 2), n // 2) if s == 3 else pl.ds(0, n)
        ref = xall.at[t, part]
        return remote(ref, ref, ag_s.at[d, s, kk], ag_r.at[d, s, kk], ahead[d])

    def ag_z(j, t):
        ref = xall.at[t, pl.ds(0, RA)]
        return remote(ref, ref, agz_s.at[j], agz_r.at[j], plane[j])

    def ag_b(j, m, t):
        ref = xall.at[t, pl.ds(RA, B - RA)]
        return remote(ref, ref, agb_s.at[j, m], agb_r.at[j, m], plane[j])

    loads[0].wait()
    for j in range(2):
        ag_z(j, me).start()
    for d in range(2):
        ag_y(d, 0, 0, me).start()
    for j in range(2):
        ag_b(j, 0, me).start()

    row = lax.broadcasted_iota(jnp.int32, (B, B), 0)
    col = lax.broadcasted_iota(jnp.int32, (B, B), 1)
    for load in loads[1:4]:
        load.wait()

    def probs(h):
        cols = slice(h * HD, (h + 1) * HD)
        scores = dot(q[:, cols], k[:, cols], 1, 1) * SCALE
        scores = jnp.where(row >= col, scores, -jnp.inf)
        e = jnp.exp(scores - jnp.max(scores, axis=-1, keepdims=True))
        a = e / jnp.sum(e, axis=-1, keepdims=True)
        att[h] = a
        gv[:, cols] = dot(a.astype(BF16), ga[:, cols], 0, 0).astype(BF16)

    probs(0)
    for j in range(2):
        t = near(j + 1) * Y + y
        ag_z(j, t).wait_recv()
        for d in range(2):
            ag_y(d, 0, j + 1, t).start()
    probs(1)
    vals[...] = jnp.zeros_like(vals)
    loads[4].wait()

    def consume(t):
        rows = pl.ds(pl.multiple_of(t * B, B), B)
        vals[...] += dot(xall[t], w[rows], 1, 0)
        term = dot(xall[t], gv[...], 0, 0).astype(BF16)
        wt[pl.ds(t * 4, 4)] = term.reshape(4, 64, B)

    def consume_at(kk, m):
        t = near(kk) * Y + up(y, m, Y)
        if kk:
            ag_b(kk - 1, m, t).wait_recv()
        consume(t)

    def far(kk):
        return up(zl, kk + 1, ZL)

    def share(t):
        rows = pl.ds(pl.multiple_of(t * B, B), B)
        return dot(gv[...], w[rows], 1, 1)

    def rs_half(d, kk):
        return remote(
            s4_out.at[d, kk], s4_in.at[d, kk], rs_s.at[d, 0, kk], rs_r.at[d, 0, kk], ahead[d]
        )

    def rs_full(d, n, kk):
        return remote(
            rs_out.at[d, n, kk], rs_in.at[d, n, kk],
            rs_s.at[d, n + 1, kk], rs_r.at[d, n + 1, kk], ahead[d],
        )

    def rs_z(j):
        return remote(tz_out.at[j], tz_in.at[j], tz_s.at[j], tz_r.at[j], plane[j])

    def rs_first(kk, carry):
        p = share(far(kk) * Y + up(y, 4, Y)).astype(BF16)
        for d in range(2):
            s4_out[d, kk] = p[d * H : (d + 1) * H]
            rs_half(d, kk).start()
        return carry

    def ring(s, carry):
        reach = (Y - 1 - s, s + 1)
        before = (lax.rem(Y - s, Y), s)
        for kk in range(ZL):
            for d in range(2):
                t = near(kk) * Y + up(y, reach[d], Y)
                for step in range(3):

                    @pl.when(s == step)
                    def _():
                        ag_y(d, step, kk, t).wait_recv()
                        ag_y(d, step + 1, kk, t).start()

                if kk == 0:
                    for j in range(2):
                        ag_b(j, reach[d], t).start()
            if kk < 2:
                consume_at(kk + 1, before[0])

                @pl.when(s > 0)
                def _():
                    consume_at(kk + 1, before[1])
            else:
                for d in range(2):
                    consume_at(0, reach[d])

                @pl.when(s == 0)
                def _():
                    consume_at(0, 0)
        return carry

    lax.fori_loop(0, 3, ring, 0)

    def rs_chunk(n, kk):
        step = 3 - n
        for d in range(2):
            acc[d][...] = share(far(kk) * Y + up(y, step if d == 0 else -step, Y))
        for d in range(2):
            if n == 0:
                rs_half(d, kk).wait_recv()
                part = slice(d * H, (d + 1) * H)
                acc[d][part] += s4_in[d, kk].astype(F32)
                rs_out[d, n, kk] = acc[d][...].astype(BF16)
            else:
                rs_full(d, n - 1, kk).wait_recv()
                rs_out[d, n, kk] = (acc[d][...] + rs_in[d, n - 1, kk].astype(F32)).astype(BF16)
            rs_full(d, n, kk).start()

    def arrived(kk):
        t = near(kk) * Y + up(y, 4, Y)
        for d in range(2):
            ag_y(d, 3, kk, t).wait_recv()
        if kk == 0:
            for j in range(2):
                ag_b(j, 4, t).start()

    lax.fori_loop(0, ZL, rs_first, 0)
    arrived(0)
    for kk in (1, 2):
        for m in (5, 3):
            consume_at(kk, m)
    rs_chunk(0, 0)
    rs_chunk(0, 1)
    consume_at(0, 4)
    for kk in (1, 2):
        arrived(kk)
        consume_at(kk, 4)

    def c_send(i):
        other = (2 * i + 1 - c) * 3
        return remote(wt.at[pl.ds(other, 3)], crecv.at[i], c_s.at[i], c_r.at[i], partner)

    def x_first(h, d):
        return remote(
            abuf.at[h, pl.ds(2 * d, 2), up(xx, 2, X)], xr1.at[h, d],
            x1_s.at[h, d], x1_r.at[h, d], x_side[d],
        )

    def x_second(h, d):
        return remote(
            abuf.at[h, :, x_side[d]["x"]], xr2.at[h, d], x2_s.at[h, d], x2_r.at[h, d], x_side[d]
        )

    def z_first(h, d):
        return remote(
            bbuf.at[h, up(zh, 2, ZH), :, pl.ds(32 * d, 32)], zr1.at[h, d],
            z1_s.at[h, d], z1_r.at[h, d], z_side[d],
        )

    def z_second(h, d):
        return remote(
            bbuf.at[h, z_side[d]["zh"]], zr2.at[h, d], z2_s.at[h, d], z2_r.at[h, d], z_side[d]
        )

    def place(j):
        return lax.rem(j, ZH), up(xx, 2 + j // ZH, X)

    def cores(j, carry):
        m, to = place(j)
        c_send(m * X + to).start()
        return carry

    lax.fori_loop(0, ZH * X, cores, 0)

    def pair_sum(j, carry):
        m, to = place(j)
        i = m * X + to
        c_send(i).wait_recv()
        mine = wt[pl.ds((2 * i + c) * 3, 3)].astype(F32)
        pair = (mine + crecv[i].astype(F32)).astype(BF16)
        for h in range(2):
            abuf[h, m, to] = pair[:, :, h * H : (h + 1) * H]
        return carry

    lax.fori_loop(0, ZH, pair_sum, 0)
    for h in range(2):
        for d in range(2):
            x_first(h, d).start()
    rs_chunk(1, 0)
    rs_chunk(1, 1)
    lax.fori_loop(ZH, ZH * X, pair_sum, 0)

    def grads(h):
        cols = slice(h * HD, (h + 1) * HD)
        a = att[h]
        gp = dot(ga[:, cols], vals[:, cols].astype(BF16), 1, 1)
        rd = jnp.sum(a * gp, axis=-1, keepdims=True)
        gs = (a * (gp - rd) * SCALE).astype(BF16)
        gq_ref[:, cols] = dot(gs, k[:, cols], 1, 0).astype(BF16)
        gk_ref[:, cols] = dot(gs, q[:, cols], 0, 0).astype(BF16)

    def x_relay(h):
        for d in range(2):
            x_first(h, d).wait_recv()
            to = x_side[d]["x"]
            for half in range(2):
                m = 2 * d + half
                abuf[h, m, to] = (
                    abuf[h, m, to].astype(F32) + xr1[h, d, half].astype(F32)
                ).astype(BF16)
            x_second(h, d).start()

    def x_sum(h):
        for d in range(2):
            x_second(h, d).wait_recv()

        def body(m, carry):
            total = abuf[h, m, xx].astype(F32) + xr2[h, 0, m].astype(F32)
            bbuf[h, m] = (total + xr2[h, 1, m].astype(F32)).astype(BF16)
            return carry

        lax.fori_loop(0, ZH, body, 0)
        for d in range(2):
            z_first(h, d).start()

    def z_relay(h):
        for d in range(2):
            z_first(h, d).wait_recv()
            to = z_side[d]["zh"]
            part = slice(32 * d, 32 * (d + 1))
            bbuf[h, to, :, part] = (
                bbuf[h, to, :, part].astype(F32) + zr1[h, d].astype(F32)
            ).astype(BF16)
            z_second(h, d).start()

    def z_sum(h):
        for d in range(2):
            z_second(h, d).wait_recv()
        total = bbuf[h, zh].astype(F32) + zr2[h, 0].astype(F32) + zr2[h, 1].astype(F32)
        gw_ref[:, h * H : (h + 1) * H] = (total * F32(1.0 / (ZH * X * C))).reshape(192, H)

    def rs_last(kk):
        acc0[...] = share(far(kk) * Y + y)
        for d in range(2):
            rs_full(d, 2, kk).wait_recv()
        total = acc0[...] + rs_in[0, 2, kk].astype(F32) + rs_in[1, 2, kk].astype(F32)
        if kk < 2:
            tz_out[kk] = total.astype(BF16)
            rs_z(kk).start()
        else:
            acc0[...] = total

    rs_chunk(0, 2)
    x_relay(0)
    rs_chunk(2, 0)
    x_relay(1)
    rs_chunk(2, 1)
    grads(0)
    rs_chunk(1, 2)
    x_sum(0)
    rs_last(0)
    x_sum(1)
    rs_last(1)
    z_relay(0)
    rs_chunk(2, 2)
    grads(1)
    z_relay(1)
    rs_last(2)
    z_sum(0)
    for j in range(2):
        rs_z(j).wait_recv()
    gi_ref[...] = (acc0[...] + tz_in[0].astype(F32) + tz_in[1].astype(F32)).astype(BF16)

    z_sum(1)

    for j in range(2):
        ag_z(j, me).wait_send()
        rs_z(j).wait_send()
    for d in range(2):
        for h in range(2):
            x_first(h, d).wait_send()
            x_second(h, d).wait_send()
            z_first(h, d).wait_send()
            z_second(h, d).wait_send()

    for d in range(2):
        for kk in range(ZL):
            for s in range(4):
                ag_y(d, s, kk, me).wait_send()

    def b_sent(m, carry):
        for j in range(2):
            ag_b(j, m, me).wait_send()
        return carry

    lax.fori_loop(0, Y, b_sent, 0)

    def sent(kk, carry):
        for d in range(2):
            for s in range(3):
                rs_full(d, s, kk).wait_send()
            rs_half(d, kk).wait_send()
        return carry

    lax.fori_loop(0, ZL, sent, 0)

    def pair_sent(i, carry):
        c_send(i).wait_send()
        return carry

    lax.fori_loop(0, ZH * X, pair_sent, 0)


def on_device(saved_input, queries, keys, value_weight, grad_attended):
    hbm = pl.BlockSpec(memory_space=pltpu.HBM)
    vmem = pl.BlockSpec(memory_space=pltpu.VMEM)
    dma = pltpu.SemaphoreType.DMA
    outs = pl.pallas_call(
        kernel,
        out_shape=(
            jax.ShapeDtypeStruct((B, B), BF16),
            jax.ShapeDtypeStruct((192, B), F32),
            jax.ShapeDtypeStruct((B, B), BF16),
            jax.ShapeDtypeStruct((B, B), BF16),
        ),
        in_specs=[hbm] * 5,
        out_specs=(vmem,) * 4,
        scratch_shapes=[
            pltpu.VMEM((T, B, B), BF16),
            pltpu.VMEM((T * B, B), BF16),
            pltpu.VMEM((B, B), BF16),
            pltpu.VMEM((B, B), BF16),
            pltpu.VMEM((B, B), BF16),
            pltpu.VMEM((B, B), BF16),
            pltpu.VMEM((HEADS, B, B), F32),
            pltpu.VMEM((B, B), F32),
            pltpu.VMEM((B, B), F32),
            pltpu.VMEM((B, B), F32),
            pltpu.VMEM((T * 4, 64, B), BF16),
            pltpu.VMEM((ZH * X, 3, 64, B), BF16),
            pltpu.VMEM((2, ZH, X, 3, 64, H), BF16),
            pltpu.VMEM((2, 2, 2, 3, 64, H), BF16),
            pltpu.VMEM((2, 2, ZH, 3, 64, H), BF16),
            pltpu.VMEM((2, ZH, 3, 64, H), BF16),
            pltpu.VMEM((2, 2, 3, 32, H), BF16),
            pltpu.VMEM((2, 2, 3, 64, H), BF16),
            pltpu.VMEM((2, ZL, H, B), BF16),
            pltpu.VMEM((2, ZL, H, B), BF16),
            pltpu.VMEM((2, 3, ZL, B, B), BF16),
            pltpu.VMEM((2, 3, ZL, B, B), BF16),
            pltpu.VMEM((2, B, B), BF16),
            pltpu.VMEM((2, B, B), BF16),
            dma((5,)),
            dma((2,)), dma((2,)), dma((2, Y)), dma((2, Y)),
            dma((2, 4, ZL)), dma((2, 4, ZL)),
            dma((2, 4, ZL)), dma((2, 4, ZL)),
            dma((2,)), dma((2,)),
            dma((ZH * X,)), dma((ZH * X,)),
            dma((2, 2)), dma((2, 2)), dma((2, 2)), dma((2, 2)),
            dma((2, 2)), dma((2, 2)), dma((2, 2)), dma((2, 2)),
        ],
        compiler_params=pltpu.CompilerParams(
            collective_id=0, has_side_effects=True, vmem_limit_bytes=67_043_328
        ),
    )(saved_input, queries, keys, value_weight, grad_attended)
    return outs


def solution(mesh):
    torus = Mesh(mesh.devices.reshape(ZH, X, C, ZL, Y), AXES)
    rows, cols = ("zh", "x", "c"), ("zl", "y")
    placed = (P(rows, cols), P(rows, cols), P(rows, cols), P(None, cols), P(rows, cols))
    return jax.shard_map(
        on_device,
        mesh=torus,
        in_specs=placed,
        out_specs=(P(rows, cols),) * 4,
        check_vma=False,
    )
```

```python
import math

import jax
import jax.numpy as jnp
from jax import lax
from jax.experimental import pallas as pl
from jax.experimental.pallas import tpu as pltpu
from jax.sharding import Mesh
from jax.sharding import PartitionSpec as P

HD = 128
HEADS = 2
ZH, X, C, ZL, Y = 4, 4, 2, 3, 8
AXES = ("zh", "x", "c", "zl", "y")
T = ZL * Y
B = 256
H = B // 2
RA = 128
MESH = pl.DeviceIdType.MESH
F32 = jnp.float32
BF16 = jnp.bfloat16
SCALE = 1.0 / math.sqrt(HD)


def dot(a, b, ca, cb):
    return lax.dot_general(a, b, (((ca,), (cb,)), ((), ())), preferred_element_type=F32)


def kernel(
    x_hbm, q_hbm, k_hbm, w_hbm, ga_hbm,
    gi_ref, gw_ref, gq_ref, gk_ref,
    xall, w, q, k, ga, gv, att, vals, acc0, acc1,
    wt, crecv, abuf, xr1, xr2, bbuf, zr1, zr2,
    s4_out, s4_in, rs_out, rs_in, tz_out, tz_in,
    in_sem, agz_s, agz_r, agb_s, agb_r, ag_s, ag_r, rs_s, rs_r, tz_s, tz_r,
    c_s, c_r, x1_s, x1_r, x2_s, x2_r, z1_s, z1_r, z2_s, z2_r,
):
    zh, xx, c, zl, y = (lax.axis_index(a) for a in AXES)
    me = zl * Y + y
    acc = (acc0, acc1)

    def up(value, step, size):
        return lax.rem(value + (step + size), size)

    ahead = ({"y": up(y, 1, Y)}, {"y": up(y, -1, Y)})
    x_side = ({"x": up(xx, 1, X)}, {"x": up(xx, -1, X)})
    z_side = ({"zh": up(zh, 1, ZH)}, {"zh": up(zh, -1, ZH)})
    plane = ({"zl": up(zl, 1, ZL)}, {"zl": up(zl, 2, ZL)})
    partner = {"c": 1 - c}

    def remote(src, dst, send, recv, where):
        return pltpu.make_async_remote_copy(
            src_ref=src, dst_ref=dst, send_sem=send, recv_sem=recv,
            device_id=where, device_id_type=MESH,
        )

    loads = [
        pltpu.make_async_copy(x_hbm, xall.at[me], in_sem.at[0]),
        pltpu.make_async_copy(q_hbm, q, in_sem.at[1]),
        pltpu.make_async_copy(k_hbm, k, in_sem.at[2]),
        pltpu.make_async_copy(ga_hbm, ga, in_sem.at[3]),
        pltpu.make_async_copy(w_hbm, w, in_sem.at[4]),
    ]
    for load in loads:
        load.start()

    barrier = pltpu.get_barrier_semaphore()
    friends = (*ahead, *x_side, *z_side, *plane, partner)
    for friend in friends:
        pl.semaphore_signal(barrier, inc=1, device_id=friend, device_id_type=MESH)
    pl.semaphore_wait(barrier, len(friends))

    def near(kk):
        return up(zl, -kk, ZL)

    def ag_y(d, s, kk, t):
        n = B if kk == 0 else RA
        part = pl.ds(d * (n // 2), n // 2) if s == 3 else pl.ds(0, n)
        ref = xall.at[t, part]
        return remote(ref, ref, ag_s.at[d, s, kk], ag_r.at[d, s, kk], ahead[d])

    def ag_z(j, t):
        ref = xall.at[t, pl.ds(0, RA)]
        return remote(ref, ref, agz_s.at[j], agz_r.at[j], plane[j])

    def ag_b(j, m, t):
        ref = xall.at[t, pl.ds(RA, B - RA)]
        return remote(ref, ref, agb_s.at[j, m], agb_r.at[j, m], plane[j])

    loads[0].wait()
    for j in range(2):
        ag_z(j, me).start()
    for d in range(2):
        ag_y(d, 0, 0, me).start()
    for j in range(2):
        ag_b(j, 0, me).start()

    row = lax.broadcasted_iota(jnp.int32, (B, B), 0)
    col = lax.broadcasted_iota(jnp.int32, (B, B), 1)
    for load in loads[1:4]:
        load.wait()

    def probs(h):
        cols = slice(h * HD, (h + 1) * HD)
        scores = dot(q[:, cols], k[:, cols], 1, 1) * SCALE
        scores = jnp.where(row >= col, scores, -jnp.inf)
        e = jnp.exp(scores - jnp.max(scores, axis=-1, keepdims=True))
        a = e / jnp.sum(e, axis=-1, keepdims=True)
        att[h] = a
        gv[:, cols] = dot(a.astype(BF16), ga[:, cols], 0, 0).astype(BF16)

    probs(0)
    for j in range(2):
        t = near(j + 1) * Y + y
        ag_z(j, t).wait_recv()
        for d in range(2):
            ag_y(d, 0, j + 1, t).start()
    probs(1)
    vals[...] = jnp.zeros_like(vals)
    loads[4].wait()

    def consume(t):
        rows = pl.ds(pl.multiple_of(t * B, B), B)
        vals[...] += dot(xall[t], w[rows], 1, 0)
        term = dot(xall[t], gv[...], 0, 0).astype(BF16)
        wt[pl.ds(t * 4, 4)] = term.reshape(4, 64, B)

    def consume_at(kk, m):
        t = near(kk) * Y + up(y, m, Y)
        if kk:
            ag_b(kk - 1, m, t).wait_recv()
        consume(t)

    def far(kk):
        return up(zl, kk + 1, ZL)

    def share(t):
        rows = pl.ds(pl.multiple_of(t * B, B), B)
        return dot(gv[...], w[rows], 1, 1)

    def rs_half(d, kk):
        return remote(
            s4_out.at[d, kk], s4_in.at[d, kk], rs_s.at[d, 0, kk], rs_r.at[d, 0, kk], ahead[d]
        )

    def rs_full(d, n, kk):
        return remote(
            rs_out.at[d, n, kk], rs_in.at[d, n, kk],
            rs_s.at[d, n + 1, kk], rs_r.at[d, n + 1, kk], ahead[d],
        )

    def rs_z(j):
        return remote(tz_out.at[j], tz_in.at[j], tz_s.at[j], tz_r.at[j], plane[j])

    def rs_first(kk, carry):
        p = share(far(kk) * Y + up(y, 4, Y)).astype(BF16)
        for d in range(2):
            s4_out[d, kk] = p[d * H : (d + 1) * H]
            rs_half(d, kk).start()
        return carry

    def ring(s, carry):
        reach = (Y - 1 - s, s + 1)
        before = (lax.rem(Y - s, Y), s)
        for kk in range(ZL):
            for d in range(2):
                t = near(kk) * Y + up(y, reach[d], Y)
                for step in range(3):

                    @pl.when(s == step)
                    def _():
                        ag_y(d, step, kk, t).wait_recv()
                        ag_y(d, step + 1, kk, t).start()

                if kk == 0:
                    for j in range(2):
                        ag_b(j, reach[d], t).start()
            if kk < 2:
                consume_at(kk + 1, before[0])

                @pl.when(s > 0)
                def _():
                    consume_at(kk + 1, before[1])
            else:
                for d in range(2):
                    consume_at(0, reach[d])

                @pl.when(s == 0)
                def _():
                    consume_at(0, 0)
        return carry

    lax.fori_loop(0, 3, ring, 0)

    def rs_chunk(n, kk):
        step = 3 - n
        for d in range(2):
            acc[d][...] = share(far(kk) * Y + up(y, step if d == 0 else -step, Y))
        for d in range(2):
            if n == 0:
                rs_half(d, kk).wait_recv()
                part = slice(d * H, (d + 1) * H)
                acc[d][part] += s4_in[d, kk].astype(F32)
                rs_out[d, n, kk] = acc[d][...].astype(BF16)
            else:
                rs_full(d, n - 1, kk).wait_recv()
                rs_out[d, n, kk] = (acc[d][...] + rs_in[d, n - 1, kk].astype(F32)).astype(BF16)
            rs_full(d, n, kk).start()

    def arrived(kk):
        t = near(kk) * Y + up(y, 4, Y)
        for d in range(2):
            ag_y(d, 3, kk, t).wait_recv()
        if kk == 0:
            for j in range(2):
                ag_b(j, 4, t).start()

    lax.fori_loop(0, ZL, rs_first, 0)
    arrived(0)
    for kk in (1, 2):
        for m in (5, 3):
            consume_at(kk, m)
    rs_chunk(0, 0)
    rs_chunk(0, 1)
    consume_at(0, 4)
    for kk in (1, 2):
        arrived(kk)
        consume_at(kk, 4)

    def c_send(i):
        other = (2 * i + 1 - c) * 3
        return remote(wt.at[pl.ds(other, 3)], crecv.at[i], c_s.at[i], c_r.at[i], partner)

    def x_first(h, d):
        return remote(
            abuf.at[h, pl.ds(2 * d, 2), up(xx, 2, X)], xr1.at[h, d],
            x1_s.at[h, d], x1_r.at[h, d], x_side[d],
        )

    def x_second(h, d):
        return remote(
            abuf.at[h, :, x_side[d]["x"]], xr2.at[h, d], x2_s.at[h, d], x2_r.at[h, d], x_side[d]
        )

    def z_first(h, d):
        return remote(
            bbuf.at[h, up(zh, 2, ZH), :, pl.ds(32 * d, 32)], zr1.at[h, d],
            z1_s.at[h, d], z1_r.at[h, d], z_side[d],
        )

    def z_second(h, d):
        return remote(
            bbuf.at[h, z_side[d]["zh"]], zr2.at[h, d], z2_s.at[h, d], z2_r.at[h, d], z_side[d]
        )

    def place(j):
        return lax.rem(j, ZH), up(xx, 2 + j // ZH, X)

    def cores(j, carry):
        m, to = place(j)
        c_send(m * X + to).start()
        return carry

    lax.fori_loop(0, ZH * X, cores, 0)

    def pair_sum(j, carry):
        m, to = place(j)
        i = m * X + to
        c_send(i).wait_recv()
        mine = wt[pl.ds((2 * i + c) * 3, 3)].astype(F32)
        pair = (mine + crecv[i].astype(F32)).astype(BF16)
        for h in range(2):
            abuf[h, m, to] = pair[:, :, h * H : (h + 1) * H]
        return carry

    lax.fori_loop(0, ZH, pair_sum, 0)
    for h in range(2):
        for d in range(2):
            x_first(h, d).start()
    rs_chunk(1, 0)
    rs_chunk(1, 1)
    lax.fori_loop(ZH, ZH * X, pair_sum, 0)

    def grads(h):
        cols = slice(h * HD, (h + 1) * HD)
        a = att[h]
        gp = dot(ga[:, cols], vals[:, cols].astype(BF16), 1, 1)
        rd = jnp.sum(a * gp, axis=-1, keepdims=True)
        gs = (a * (gp - rd) * SCALE).astype(BF16)
        gq_ref[:, cols] = dot(gs, k[:, cols], 1, 0).astype(BF16)
        gk_ref[:, cols] = dot(gs, q[:, cols], 0, 0).astype(BF16)

    def x_relay(h):
        for d in range(2):
            x_first(h, d).wait_recv()
            to = x_side[d]["x"]
            for half in range(2):
                m = 2 * d + half
                abuf[h, m, to] = (
                    abuf[h, m, to].astype(F32) + xr1[h, d, half].astype(F32)
                ).astype(BF16)
            x_second(h, d).start()

    def x_sum(h):
        for d in range(2):
            x_second(h, d).wait_recv()

        def body(m, carry):
            total = abuf[h, m, xx].astype(F32) + xr2[h, 0, m].astype(F32)
            bbuf[h, m] = (total + xr2[h, 1, m].astype(F32)).astype(BF16)
            return carry

        lax.fori_loop(0, ZH, body, 0)
        for d in range(2):
            z_first(h, d).start()

    def z_relay(h):
        for d in range(2):
            z_first(h, d).wait_recv()
            to = z_side[d]["zh"]
            part = slice(32 * d, 32 * (d + 1))
            bbuf[h, to, :, part] = (
                bbuf[h, to, :, part].astype(F32) + zr1[h, d].astype(F32)
            ).astype(BF16)
            z_second(h, d).start()

    def z_sum(h):
        for d in range(2):
            z_second(h, d).wait_recv()
        total = bbuf[h, zh].astype(F32) + zr2[h, 0].astype(F32) + zr2[h, 1].astype(F32)
        gw_ref[:, h * H : (h + 1) * H] = (total * F32(1.0 / (ZH * X * C))).reshape(192, H)

    def rs_last(kk):
        acc0[...] = share(far(kk) * Y + y)
        for d in range(2):
            rs_full(d, 2, kk).wait_recv()
        total = acc0[...] + rs_in[0, 2, kk].astype(F32) + rs_in[1, 2, kk].astype(F32)
        if kk < 2:
            tz_out[kk] = total.astype(BF16)
            rs_z(kk).start()
        else:
            acc0[...] = total

    rs_chunk(0, 2)
    x_relay(0)
    rs_chunk(2, 0)
    x_relay(1)
    rs_chunk(2, 1)
    grads(0)
    rs_chunk(1, 2)
    x_sum(0)
    rs_last(0)
    x_sum(1)
    rs_last(1)
    z_relay(0)
    rs_chunk(2, 2)
    grads(1)
    z_relay(1)
    rs_last(2)
    z_sum(0)
    for j in range(2):
        rs_z(j).wait_recv()
    gi_ref[...] = (acc0[...] + tz_in[0].astype(F32) + tz_in[1].astype(F32)).astype(BF16)

    z_sum(1)

    for j in range(2):
        ag_z(j, me).wait_send()
        rs_z(j).wait_send()
    for d in range(2):
        for h in range(2):
            x_first(h, d).wait_send()
            x_second(h, d).wait_send()
            z_first(h, d).wait_send()
            z_second(h, d).wait_send()

    for d in range(2):
        for kk in range(ZL):
            for s in range(4):
                ag_y(d, s, kk, me).wait_send()

    def b_sent(m, carry):
        for j in range(2):
            ag_b(j, m, me).wait_send()
        return carry

    lax.fori_loop(0, Y, b_sent, 0)

    def sent(kk, carry):
        for d in range(2):
            for s in range(3):
                rs_full(d, s, kk).wait_send()
            rs_half(d, kk).wait_send()
        return carry

    lax.fori_loop(0, ZL, sent, 0)

    def pair_sent(i, carry):
        c_send(i).wait_send()
        return carry

    lax.fori_loop(0, ZH * X, pair_sent, 0)


def on_device(saved_input, queries, keys, value_weight, grad_attended):
    hbm = pl.BlockSpec(memory_space=pltpu.HBM)
    vmem = pl.BlockSpec(memory_space=pltpu.VMEM)
    dma = pltpu.SemaphoreType.DMA
    outs = pl.pallas_call(
        kernel,
        out_shape=(
            pltpu.VMEM((B, B), BF16),
            pltpu.VMEM((192, B), F32),
            pltpu.VMEM((B, B), BF16),
            pltpu.VMEM((B, B), BF16),
        ),
        in_specs=[hbm] * 5,
        out_specs=(vmem,) * 4,
        scratch_shapes=[
            pltpu.VMEM((T, B, B), BF16),
            pltpu.VMEM((T * B, B), BF16),
            pltpu.VMEM((B, B), BF16),
            pltpu.VMEM((B, B), BF16),
            pltpu.VMEM((B, B), BF16),
            pltpu.VMEM((B, B), BF16),
            pltpu.VMEM((HEADS, B, B), F32),
            pltpu.VMEM((B, B), F32),
            pltpu.VMEM((B, B), F32),
            pltpu.VMEM((B, B), F32),
            pltpu.VMEM((T * 4, 64, B), BF16),
            pltpu.VMEM((ZH * X, 3, 64, B), BF16),
            pltpu.VMEM((2, ZH, X, 3, 64, H), BF16),
            pltpu.VMEM((2, 2, 2, 3, 64, H), BF16),
            pltpu.VMEM((2, 2, ZH, 3, 64, H), BF16),
            pltpu.VMEM((2, ZH, 3, 64, H), BF16),
            pltpu.VMEM((2, 2, 3, 32, H), BF16),
            pltpu.VMEM((2, 2, 3, 64, H), BF16),
            pltpu.VMEM((2, ZL, H, B), BF16),
            pltpu.VMEM((2, ZL, H, B), BF16),
            pltpu.VMEM((2, 3, ZL, B, B), BF16),
            pltpu.VMEM((2, 3, ZL, B, B), BF16),
            pltpu.VMEM((2, B, B), BF16),
            pltpu.VMEM((2, B, B), BF16),
            dma((5,)),
            dma((2,)), dma((2,)), dma((2, Y)), dma((2, Y)),
            dma((2, 4, ZL)), dma((2, 4, ZL)),
            dma((2, 4, ZL)), dma((2, 4, ZL)),
            dma((2,)), dma((2,)),
            dma((ZH * X,)), dma((ZH * X,)),
            dma((2, 2)), dma((2, 2)), dma((2, 2)), dma((2, 2)),
            dma((2, 2)), dma((2, 2)), dma((2, 2)), dma((2, 2)),
        ],
        compiler_params=pltpu.CompilerParams(
            collective_id=0, has_side_effects=True, vmem_limit_bytes=66_400_000
        ),
    )(saved_input, queries, keys, value_weight, grad_attended)
    return outs


def solution(mesh):
    torus = Mesh(mesh.devices.reshape(ZH, X, C, ZL, Y), AXES)
    rows, cols = ("zh", "x", "c"), ("zl", "y")
    placed = (P(rows, cols), P(rows, cols), P(rows, cols), P(None, cols), P(rows, cols))
    return jax.shard_map(
        on_device,
        mesh=torus,
        in_specs=placed,
        out_specs=(P(rows, cols),) * 4,
        check_vma=False,
    )
```

```python
import math

import jax
import jax.numpy as jnp
from jax import lax
from jax.experimental import pallas as pl
from jax.experimental.pallas import tpu as pltpu
from jax.sharding import Mesh
from jax.sharding import PartitionSpec as P

HD = 128
HEADS = 2
ZH, X, C, ZL, Y = 4, 4, 2, 3, 8
AXES = ("zh", "x", "c", "zl", "y")
T = ZL * Y
B = 256
H = B // 2
RA = 128
MESH = pl.DeviceIdType.MESH
F32 = jnp.float32
BF16 = jnp.bfloat16
SCALE = 1.0 / math.sqrt(HD)


def dot(a, b, ca, cb):
    return lax.dot_general(a, b, (((ca,), (cb,)), ((), ())), preferred_element_type=F32)


def kernel(
    x_hbm, q_hbm, k_hbm, w_hbm, ga_hbm,
    gi_ref, gw_ref, gq_ref, gk_ref,
    xall, w, q, k, ga, gv, att, vals, acc0, acc1,
    wt, crecv, abuf, xr1, xr2, bbuf, zr1, zr2,
    s4_out, s4_in, rs_out, rs_in, tz_out, tz_in,
    in_sem, agz_s, agz_r, agb_s, agb_r, ag_s, ag_r, rs_s, rs_r, tz_s, tz_r,
    c_s, c_r, x1_s, x1_r, x2_s, x2_r, z1_s, z1_r, z2_s, z2_r,
):
    zh, xx, c, zl, y = (lax.axis_index(a) for a in AXES)
    me = zl * Y + y
    acc = (acc0, acc1)

    def up(value, step, size):
        return lax.rem(value + (step + size), size)

    ahead = ({"y": up(y, 1, Y)}, {"y": up(y, -1, Y)})
    x_side = ({"x": up(xx, 1, X)}, {"x": up(xx, -1, X)})
    z_side = ({"zh": up(zh, 1, ZH)}, {"zh": up(zh, -1, ZH)})
    plane = ({"zl": up(zl, 1, ZL)}, {"zl": up(zl, 2, ZL)})
    partner = {"c": 1 - c}

    def remote(src, dst, send, recv, where):
        return pltpu.make_async_remote_copy(
            src_ref=src, dst_ref=dst, send_sem=send, recv_sem=recv,
            device_id=where, device_id_type=MESH,
        )

    loads = [
        pltpu.make_async_copy(x_hbm, xall.at[me], in_sem.at[0]),
        pltpu.make_async_copy(q_hbm, q, in_sem.at[1]),
        pltpu.make_async_copy(k_hbm, k, in_sem.at[2]),
        pltpu.make_async_copy(ga_hbm, ga, in_sem.at[3]),
        pltpu.make_async_copy(w_hbm, w, in_sem.at[4]),
    ]
    for load in loads:
        load.start()

    barrier = pltpu.get_barrier_semaphore()
    friends = (*ahead, *x_side, *z_side, *plane, partner)
    for friend in friends:
        pl.semaphore_signal(barrier, inc=1, device_id=friend, device_id_type=MESH)
    pl.semaphore_wait(barrier, len(friends))

    def near(kk):
        return up(zl, -kk, ZL)

    def ag_y(d, s, kk, t):
        n = B if kk == 0 else RA
        part = pl.ds(d * (n // 2), n // 2) if s == 3 else pl.ds(0, n)
        ref = xall.at[t, part]
        return remote(ref, ref, ag_s.at[d, s, kk], ag_r.at[d, s, kk], ahead[d])

    def ag_z(j, t):
        ref = xall.at[t, pl.ds(0, RA)]
        return remote(ref, ref, agz_s.at[j], agz_r.at[j], plane[j])

    def ag_b(j, m, t):
        ref = xall.at[t, pl.ds(RA, B - RA)]
        return remote(ref, ref, agb_s.at[j, m], agb_r.at[j, m], plane[j])

    loads[0].wait()
    for j in range(2):
        ag_z(j, me).start()
    for d in range(2):
        ag_y(d, 0, 0, me).start()
    for j in range(2):
        ag_b(j, 0, me).start()

    row = lax.broadcasted_iota(jnp.int32, (B, B), 0)
    col = lax.broadcasted_iota(jnp.int32, (B, B), 1)
    for load in loads[1:4]:
        load.wait()

    def probs(h):
        cols = slice(h * HD, (h + 1) * HD)
        scores = dot(q[:, cols], k[:, cols], 1, 1) * SCALE
        scores = jnp.where(row >= col, scores, -jnp.inf)
        e = jnp.exp(scores - jnp.max(scores, axis=-1, keepdims=True))
        a = e / jnp.sum(e, axis=-1, keepdims=True)
        att[h] = a
        gv[:, cols] = dot(a.astype(BF16), ga[:, cols], 0, 0).astype(BF16)

    probs(0)
    for j in range(2):
        t = near(j + 1) * Y + y
        ag_z(j, t).wait_recv()
        for d in range(2):
            ag_y(d, 0, j + 1, t).start()
    probs(1)
    vals[...] = jnp.zeros_like(vals)
    loads[4].wait()

    def consume(t):
        rows = pl.ds(pl.multiple_of(t * B, B), B)
        vals[...] += dot(xall[t], w[rows], 1, 0)
        term = dot(xall[t], gv[...], 0, 0).astype(BF16)
        wt[pl.ds(t * 4, 4)] = term.reshape(4, 64, B)

    def consume_at(kk, m):
        t = near(kk) * Y + up(y, m, Y)
        if kk:
            ag_b(kk - 1, m, t).wait_recv()
        consume(t)

    def far(kk):
        return up(zl, kk + 1, ZL)

    def share(t):
        rows = pl.ds(pl.multiple_of(t * B, B), B)
        return dot(gv[...], w[rows], 1, 1)

    def rs_half(d, kk):
        return remote(
            s4_out.at[d, kk], s4_in.at[d, kk], rs_s.at[d, 0, kk], rs_r.at[d, 0, kk], ahead[d]
        )

    def rs_full(d, n, kk):
        return remote(
            rs_out.at[d, n, kk], rs_in.at[d, n, kk],
            rs_s.at[d, n + 1, kk], rs_r.at[d, n + 1, kk], ahead[d],
        )

    def rs_z(j):
        return remote(tz_out.at[j], tz_in.at[j], tz_s.at[j], tz_r.at[j], plane[j])

    def rs_first(kk, carry):
        p = share(far(kk) * Y + up(y, 4, Y)).astype(BF16)
        for d in range(2):
            s4_out[d, kk] = p[d * H : (d + 1) * H]
            rs_half(d, kk).start()
        return carry

    def ring(s, carry):
        reach = (Y - 1 - s, s + 1)
        before = (lax.rem(Y - s, Y), s)
        for kk in range(ZL):
            for d in range(2):
                t = near(kk) * Y + up(y, reach[d], Y)
                for step in range(3):

                    @pl.when(s == step)
                    def _():
                        ag_y(d, step, kk, t).wait_recv()
                        ag_y(d, step + 1, kk, t).start()

                if kk == 0:
                    for j in range(2):
                        ag_b(j, reach[d], t).start()
            if kk < 2:
                consume_at(kk + 1, before[0])

                @pl.when(s > 0)
                def _():
                    consume_at(kk + 1, before[1])
            else:
                for d in range(2):
                    consume_at(0, reach[d])

                @pl.when(s == 0)
                def _():
                    consume_at(0, 0)
        return carry

    lax.fori_loop(0, 3, ring, 0)

    def rs_chunk(n, kk):
        step = 3 - n
        for d in range(2):
            acc[d][...] = share(far(kk) * Y + up(y, step if d == 0 else -step, Y))
        for d in range(2):
            if n == 0:
                rs_half(d, kk).wait_recv()
                part = slice(d * H, (d + 1) * H)
                acc[d][part] += s4_in[d, kk].astype(F32)
                rs_out[d, n, kk] = acc[d][...].astype(BF16)
            else:
                rs_full(d, n - 1, kk).wait_recv()
                rs_out[d, n, kk] = (acc[d][...] + rs_in[d, n - 1, kk].astype(F32)).astype(BF16)
            rs_full(d, n, kk).start()

    def arrived(kk):
        t = near(kk) * Y + up(y, 4, Y)
        for d in range(2):
            ag_y(d, 3, kk, t).wait_recv()
        if kk == 0:
            for j in range(2):
                ag_b(j, 4, t).start()

    lax.fori_loop(0, ZL, rs_first, 0)
    arrived(0)
    for kk in (1, 2):
        for m in (5, 3):
            consume_at(kk, m)
    rs_chunk(0, 0)
    rs_chunk(0, 1)
    consume_at(0, 4)
    for kk in (1, 2):
        arrived(kk)
        consume_at(kk, 4)

    def c_send(i):
        other = (2 * i + 1 - c) * 3
        return remote(wt.at[pl.ds(other, 3)], crecv.at[i], c_s.at[i], c_r.at[i], partner)

    def x_first(h, d):
        return remote(
            abuf.at[h, pl.ds(2 * d, 2), up(xx, 2, X)], xr1.at[h, d],
            x1_s.at[h, d], x1_r.at[h, d], x_side[d],
        )

    def x_second(h, d):
        return remote(
            abuf.at[h, :, x_side[d]["x"]], xr2.at[h, d], x2_s.at[h, d], x2_r.at[h, d], x_side[d]
        )

    def z_first(h, d):
        return remote(
            bbuf.at[h, up(zh, 2, ZH), :, pl.ds(32 * d, 32)], zr1.at[h, d],
            z1_s.at[h, d], z1_r.at[h, d], z_side[d],
        )

    def z_second(h, d):
        return remote(
            bbuf.at[h, z_side[d]["zh"]], zr2.at[h, d], z2_s.at[h, d], z2_r.at[h, d], z_side[d]
        )

    def place(j):
        return lax.rem(j, ZH), up(xx, 2 + j // ZH, X)

    def cores(j, carry):
        m, to = place(j)
        c_send(m * X + to).start()
        return carry

    lax.fori_loop(0, ZH * X, cores, 0)

    def pair_sum(j, carry):
        m, to = place(j)
        i = m * X + to
        c_send(i).wait_recv()
        mine = wt[pl.ds((2 * i + c) * 3, 3)].astype(F32)
        pair = (mine + crecv[i].astype(F32)).astype(BF16)
        for h in range(2):
            abuf[h, m, to] = pair[:, :, h * H : (h + 1) * H]
        return carry

    lax.fori_loop(0, ZH, pair_sum, 0)
    for h in range(2):
        for d in range(2):
            x_first(h, d).start()
    rs_chunk(1, 0)
    rs_chunk(1, 1)
    lax.fori_loop(ZH, ZH * X, pair_sum, 0)

    def grads(h):
        cols = slice(h * HD, (h + 1) * HD)
        a = att[h]
        gp = dot(ga[:, cols], vals[:, cols].astype(BF16), 1, 1)
        rd = jnp.sum(a * gp, axis=-1, keepdims=True)
        gs = (a * (gp - rd) * SCALE).astype(BF16)
        gq_ref[:, cols] = dot(gs, k[:, cols], 1, 0).astype(BF16)
        gk_ref[:, cols] = dot(gs, q[:, cols], 0, 0).astype(BF16)

    def x_relay(h):
        for d in range(2):
            x_first(h, d).wait_recv()
            to = x_side[d]["x"]
            for half in range(2):
                m = 2 * d + half
                abuf[h, m, to] = (
                    abuf[h, m, to].astype(F32) + xr1[h, d, half].astype(F32)
                ).astype(BF16)
            x_second(h, d).start()

    def x_sum(h):
        for d in range(2):
            x_second(h, d).wait_recv()

        def body(m, carry):
            total = abuf[h, m, xx].astype(F32) + xr2[h, 0, m].astype(F32)
            bbuf[h, m] = (total + xr2[h, 1, m].astype(F32)).astype(BF16)
            return carry

        lax.fori_loop(0, ZH, body, 0)
        for d in range(2):
            z_first(h, d).start()

    def z_relay(h):
        for d in range(2):
            z_first(h, d).wait_recv()
            to = z_side[d]["zh"]
            part = slice(32 * d, 32 * (d + 1))
            bbuf[h, to, :, part] = (
                bbuf[h, to, :, part].astype(F32) + zr1[h, d].astype(F32)
            ).astype(BF16)
            z_second(h, d).start()

    def z_sum(h):
        for d in range(2):
            z_second(h, d).wait_recv()
        total = bbuf[h, zh].astype(F32) + zr2[h, 0].astype(F32) + zr2[h, 1].astype(F32)
        gw_ref[:, h * H : (h + 1) * H] = (total * F32(1.0 / (ZH * X * C))).reshape(192, H)

    def rs_last(kk):
        acc0[...] = share(far(kk) * Y + y)
        for d in range(2):
            rs_full(d, 2, kk).wait_recv()
        total = acc0[...] + rs_in[0, 2, kk].astype(F32) + rs_in[1, 2, kk].astype(F32)
        if kk < 2:
            tz_out[kk] = total.astype(BF16)
            rs_z(kk).start()
        else:
            acc0[...] = total

    rs_chunk(0, 2)
    x_relay(0)
    rs_chunk(2, 0)
    x_relay(1)
    rs_chunk(2, 1)
    grads(0)
    rs_chunk(1, 2)
    x_sum(0)
    rs_last(0)
    x_sum(1)
    rs_last(1)
    z_relay(0)
    rs_chunk(2, 2)
    grads(1)
    z_relay(1)
    rs_last(2)
    z_sum(0)
    for j in range(2):
        rs_z(j).wait_recv()
    gi_ref[...] = (acc0[...] + tz_in[0].astype(F32) + tz_in[1].astype(F32)).astype(BF16)

    z_sum(1)

    for j in range(2):
        ag_z(j, me).wait_send()
        rs_z(j).wait_send()
    for d in range(2):
        for h in range(2):
            x_first(h, d).wait_send()
            x_second(h, d).wait_send()
            z_first(h, d).wait_send()
            z_second(h, d).wait_send()

    for d in range(2):
        for kk in range(ZL):
            for s in range(4):
                ag_y(d, s, kk, me).wait_send()

    def b_sent(m, carry):
        for j in range(2):
            ag_b(j, m, me).wait_send()
        return carry

    lax.fori_loop(0, Y, b_sent, 0)

    def sent(kk, carry):
        for d in range(2):
            for s in range(3):
                rs_full(d, s, kk).wait_send()
            rs_half(d, kk).wait_send()
        return carry

    lax.fori_loop(0, ZL, sent, 0)

    def pair_sent(i, carry):
        c_send(i).wait_send()
        return carry

    lax.fori_loop(0, ZH * X, pair_sent, 0)


def write_out(*refs):
    sems = refs[8]
    copies = [pltpu.make_async_copy(refs[n], refs[n + 4], sems.at[n]) for n in range(4)]
    for copy in copies:
        copy.start()
    for copy in copies:
        copy.wait()


def on_device(saved_input, queries, keys, value_weight, grad_attended):
    hbm = pl.BlockSpec(memory_space=pltpu.HBM)
    vmem = pl.BlockSpec(memory_space=pltpu.VMEM)
    dma = pltpu.SemaphoreType.DMA
    outs = pl.pallas_call(
        kernel,
        out_shape=(
            pltpu.VMEM((B, B), BF16),
            pltpu.VMEM((192, B), F32),
            pltpu.VMEM((B, B), BF16),
            pltpu.VMEM((B, B), BF16),
        ),
        in_specs=[hbm] * 5,
        out_specs=(vmem,) * 4,
        scratch_shapes=[
            pltpu.VMEM((T, B, B), BF16),
            pltpu.VMEM((T * B, B), BF16),
            pltpu.VMEM((B, B), BF16),
            pltpu.VMEM((B, B), BF16),
            pltpu.VMEM((B, B), BF16),
            pltpu.VMEM((B, B), BF16),
            pltpu.VMEM((HEADS, B, B), F32),
            pltpu.VMEM((B, B), F32),
            pltpu.VMEM((B, B), F32),
            pltpu.VMEM((B, B), F32),
            pltpu.VMEM((T * 4, 64, B), BF16),
            pltpu.VMEM((ZH * X, 3, 64, B), BF16),
            pltpu.VMEM((2, ZH, X, 3, 64, H), BF16),
            pltpu.VMEM((2, 2, 2, 3, 64, H), BF16),
            pltpu.VMEM((2, 2, ZH, 3, 64, H), BF16),
            pltpu.VMEM((2, ZH, 3, 64, H), BF16),
            pltpu.VMEM((2, 2, 3, 32, H), BF16),
            pltpu.VMEM((2, 2, 3, 64, H), BF16),
            pltpu.VMEM((2, ZL, H, B), BF16),
            pltpu.VMEM((2, ZL, H, B), BF16),
            pltpu.VMEM((2, 3, ZL, B, B), BF16),
            pltpu.VMEM((2, 3, ZL, B, B), BF16),
            pltpu.VMEM((2, B, B), BF16),
            pltpu.VMEM((2, B, B), BF16),
            dma((5,)),
            dma((2,)), dma((2,)), dma((2, Y)), dma((2, Y)),
            dma((2, 4, ZL)), dma((2, 4, ZL)),
            dma((2, 4, ZL)), dma((2, 4, ZL)),
            dma((2,)), dma((2,)),
            dma((ZH * X,)), dma((ZH * X,)),
            dma((2, 2)), dma((2, 2)), dma((2, 2)), dma((2, 2)),
            dma((2, 2)), dma((2, 2)), dma((2, 2)), dma((2, 2)),
        ],
        compiler_params=pltpu.CompilerParams(
            collective_id=0, has_side_effects=True, vmem_limit_bytes=66_400_000
        ),
    )(saved_input, queries, keys, value_weight, grad_attended)
    return pl.pallas_call(
        write_out,
        out_shape=tuple(jax.ShapeDtypeStruct(o.shape, o.dtype) for o in outs),
        in_specs=[vmem] * 4,
        out_specs=(hbm,) * 4,
        scratch_shapes=[dma((4,))],
        compiler_params=pltpu.CompilerParams(vmem_limit_bytes=1024 * 1024),
    )(*outs)


def solution(mesh):
    torus = Mesh(mesh.devices.reshape(ZH, X, C, ZL, Y), AXES)
    rows, cols = ("zh", "x", "c"), ("zl", "y")
    placed = (P(rows, cols), P(rows, cols), P(rows, cols), P(None, cols), P(rows, cols))
    return jax.shard_map(
        on_device,
        mesh=torus,
        in_specs=placed,
        out_specs=(P(rows, cols),) * 4,
        check_vma=False,
    )
```
